32 devices in a mesh: dp: 8 (over z, x), rep: 4 (over y, core).
Axes of the slice: x: 2, y: 2, z: 4, core: 2. Of those that a mesh axis runs over, the one named last changes fastest.
Arguments:
- tokens: bfloat16 [65536, 1280], P(('dp', 'rep')), may hold values from -6 to 6
- sketch_map: bfloat16 [65536, 128], P(('dp', 'rep')), may hold values from -0.125 to 0.125
- test_matrix: bfloat16 [4, 1024, 128], P('rep'), may hold values from -0.09375 to 0.09375
Outputs:
- basis: float32 [1280, 128], P('dp')
- factor: float32 [128, 128], replicated
The draws below stay inside these ranges and needn't reach their ends.
All inputs are finite; a program needn't handle non-finite values.
Results may differ from the reference program's by a relative error of at most 0.0051.
Values may be sent and summed in bfloat16 or wider, within the bound.
A program may use at most 64 MiB of HBM per device.

```python
import jax
import jax.numpy as jnp
from jax import lax

D = 1280
K = 128
ITERS = 2
TOK_DEV = 2048
TOKENS = 65536
SKETCH_ROWS = 1024
N_DP = 8
N_REP = 4


def raised(entries, rng, source, target, blocks, factor):
    owner, partner = [(jnp.arange(entries.shape[dim]) // (entries.shape[dim] // blocks)).reshape([-1 if axis == dim else 1 for axis in range(entries.ndim)]) for dim in (source, target)]
    chosen = jax.random.permutation(rng, blocks)[partner]
    strong = (owner == chosen) | (owner == (partner + blocks // 2) % blocks)
    return jnp.where(strong, factor * entries, entries)


def levels(stream_key, extent, pieces, least, largest):
    factor_of = 1.0
    for position, blocks in pieces:
        draws = jax.random.uniform(jax.random.fold_in(jax.random.fold_in(stream_key, 6), position), (blocks,), jnp.float32, least / len(pieces), largest / len(pieces))
        factor_of = factor_of * jnp.repeat(jnp.exp(draws), extent[position] // blocks).reshape((-1,) + (1,) * (len(extent) - 1 - position))
    return factor_of


def centred(rng, dims, scale, limit, split=(), kind=jnp.bfloat16):
    values = jax.random.normal(rng, dims, jnp.float32) * scale
    if len(split) > 0:
        values = levels(rng, dims, split, -0.22, 0.18) * values
    return jnp.clip(values, min=-limit, max=limit).astype(kind)


def bell_draw_with(key, shape, width, most, pieces, heavy, kind=jnp.bfloat16):
    array = width * jax.random.normal(key, shape, jnp.float32)
    if pieces:
        array = array * levels(key, shape, pieces, -0.22, 0.18)
    return jnp.clip(raised(array, jax.random.fold_in(key, 3), *heavy), -most, most).astype(kind)


def setup_inputs(seed: int = 0) -> dict:
    key_list = jax.random.split(jax.random.key(seed), 4)
    tokens = bell_draw_with(key_list[0], (TOKENS, D), 1.0, 6.0, ((0, 32),), (0, 1, 32, 2.75))
    sketch_map = centred(key_list[1], (TOKENS, K), TOK_DEV ** -0.5, 0.125, ((0, 32),))
    test_matrix = centred(key_list[2], (N_REP, SKETCH_ROWS, K), (SKETCH_ROWS * N_REP) ** -0.5, 0.09375, ((0, 4),))
    return dict(tokens=tokens, sketch_map=sketch_map, test_matrix=test_matrix)


def orthonormal(matrix):
    gram = jnp.dot(matrix.T.astype(jnp.float32), matrix.astype(jnp.float32), precision=lax.Precision.HIGHEST, preferred_element_type=jnp.float32)
    lower = jnp.linalg.cholesky(gram)
    basis = jax.scipy.linalg.solve_triangular(lower, matrix.T, lower=True).T
    return (basis, lower.T)

def reference(tokens, sketch_map, test_matrix):
    devices = N_DP * N_REP
    slabs = tokens.reshape(devices, TOK_DEV, D)
    maps = sketch_map.reshape(devices, TOK_DEV, K)

    def one_sketch(pair):
        return lax.dot_general(pair[1].astype(jnp.float32), pair[0].astype(jnp.float32), (((0,), (0,)), ((), ())), preferred_element_type=jnp.float32).astype(jnp.bfloat16)
    sketches = lax.map(one_sketch, (slabs, maps))
    grouped = sketches.reshape(N_DP, N_REP, K, D).transpose(1, 0, 2, 3).reshape(N_REP, N_DP * K, D)
    start = jnp.zeros((D, K), jnp.float32)
    for group in range(N_REP):
        start = start + lax.dot_general(grouped[group].astype(jnp.float32), test_matrix[group].astype(jnp.float32), (((0,), (0,)), ((), ())), preferred_element_type=jnp.float32)
    current, factor = orthonormal(start)
    for step in range(ITERS):
        rounded = current.astype(jnp.bfloat16)
        projected = jnp.dot(tokens.astype(jnp.float32), rounded.astype(jnp.float32), preferred_element_type=jnp.float32).astype(jnp.bfloat16)
        summed = lax.dot_general(tokens.astype(jnp.float32), projected.astype(jnp.float32), (((0,), (0,)), ((), ())), preferred_element_type=jnp.float32)
        current, factor = orthonormal(summed / TOKENS)
    return (current, factor)
```

```python
import functools

import jax
import jax.numpy as jnp
from jax import lax
from jax.experimental import pallas as pl
from jax.experimental.pallas import tpu as pltpu
from jax.sharding import PartitionSpec as P

ITERS = 2
BLOCK = 16
SLABS = 4
LOGICAL = pl.DeviceIdType.LOGICAL
FIRST = (((0,), (0,)), ((), ()))
LAST = (((1,), (1,)), ((), ()))
EXACT = lax.Precision.HIGHEST


def when(full, condition, action):
    if full:
        action()
    else:
        pl.when(condition)(action)


def reduce_stage(n, b, g, scale, fill, greeted, z, send, pair, recv, p, ps, pr, s1, r1, s2, r2, s3, r3):
    m = n // 2
    owners, chunk, _ = send.shape
    full = owners == m
    half = owners * chunk
    me = 2 * g + b
    partner = me + 1 - 2 * b
    mine = pl.multiple_of(b * half, 8)
    theirs = pl.multiple_of((1 - b) * half, 8)

    def peer_of(k):
        peer = g + k
        return peer - jnp.where(peer >= m, m, 0)

    def source_of(k):
        peer = g - k
        return peer + jnp.where(peer < 0, m, 0)

    def rows(side, index):
        return pl.ds(pl.multiple_of(side + index * chunk, 8), chunk)

    swap = pltpu.make_async_remote_copy(
        src_ref=z.at[pl.ds(theirs, half)], dst_ref=pair, send_sem=ps, recv_sem=pr,
        device_id=partner, device_id_type=LOGICAL,
    )
    fill(theirs)
    greeted()
    swap.start()
    fill(mine)

    def scatter_copy(k, slot):
        return pltpu.make_async_remote_copy(
            src_ref=send.at[slot], dst_ref=recv.at[k], send_sem=s1.at[k], recv_sem=r1.at[k],
            device_id=2 * peer_of(k) + b, device_id_type=LOGICAL,
        )

    def gather_copy(k):
        return pltpu.make_async_remote_copy(
            src_ref=p.at[rows(mine, g)], dst_ref=p.at[rows(mine, g)], send_sem=s2.at[k], recv_sem=r2.at[k],
            device_id=2 * peer_of(k) + b, device_id_type=LOGICAL,
        )

    def forward_copy(k, index):
        return pltpu.make_async_remote_copy(
            src_ref=p.at[rows(mine, index)], dst_ref=p.at[rows(mine, index)], send_sem=s3.at[k], recv_sem=r3.at[k],
            device_id=partner, device_id_type=LOGICAL,
        )

    swap.wait_recv()

    def scatter(k, carry):
        peer = peer_of(k)

        def go():
            value = z[rows(mine, peer), :] + pair[pl.ds(pl.multiple_of(peer * chunk, 8), chunk), :]
            send[peer] = value.astype(jnp.bfloat16)
            scatter_copy(k, peer).start()

        when(full, peer < owners, go)
        return carry

    lax.fori_loop(1, m, scatter, 0)

    def own():
        total = z[rows(mine, g), :] + pair[pl.ds(pl.multiple_of(g * chunk, 8), chunk), :]

        def add(k, total):
            scatter_copy(k, 0).wait_recv()
            return total + recv[k].astype(jnp.float32)

        total = lax.fori_loop(1, m, add, total)
        p[rows(mine, g), :] = total * scale

        def gather(k, carry):
            gather_copy(k).start()
            return carry

        lax.fori_loop(1, m, gather, 0)
        forward_copy(0, g).start()

    when(full, g < owners, own)

    def collect(k, carry):
        source = source_of(k)

        def go():
            gather_copy(k).wait_recv()
            forward_copy(k, source).start()

        when(full, source < owners, go)
        return carry

    lax.fori_loop(1, m, collect, 0)

    def arrive(k, carry):
        when(full, source_of(k) < owners, lambda: forward_copy(k, 0).wait_recv())
        return carry

    lax.fori_loop(0, m, arrive, 0)

    def finish():
        swap.wait_send()

        def done(k, carry):
            when(full, peer_of(k) < owners, lambda: scatter_copy(k, 0).wait_send())
            when(full, g < owners, lambda: gather_copy(k).wait_send())
            when(full, source_of(k) < owners, lambda: forward_copy(k, 0).wait_send())
            return carry

        lax.fori_loop(1, m, done, 0)
        when(full, g < owners, lambda: forward_copy(0, 0).wait_send())

    return finish


def factorize(p, left, right):
    k = left.shape[0]
    value = p[...]
    left[...] = lax.dot_general(value, value, FIRST, precision=EXACT, preferred_element_type=jnp.float32)
    row = lax.broadcasted_iota(jnp.int32, (k, k), 0)
    col = lax.broadcasted_iota(jnp.int32, (k, k), 1)
    right[...] = jnp.where(row == col, 1.0, 0.0)
    rid = lax.broadcasted_iota(jnp.int32, (BLOCK, k), 0)
    for o in range(0, k, BLOCK):
        a = left[o : o + BLOCK, :]
        e = right[o : o + BLOCK, :]
        cols = [jnp.broadcast_to(a[:, o + t : o + t + 1], (BLOCK, k)) for t in range(BLOCK)]
        for s in range(BLOCK):
            inv = lax.rsqrt(cols[s][s : s + 1, :])
            f = jnp.where(rid > s, cols[s] * inv, 0.0)
            arow = a[s : s + 1, :] * inv
            erow = e[s : s + 1, :] * inv
            a = jnp.where(rid == s, arow, a - f * arow)
            e = jnp.where(rid == s, erow, e - f * erow)
            for t in range(s + 1, BLOCK):
                cols[t] = cols[t] - f * (cols[t][s : s + 1, :] * inv)
        left[o : o + BLOCK, :] = a
        right[o : o + BLOCK, :] = e
        if o + BLOCK < k:
            ua = lax.dot_general(a, a, FIRST, precision=EXACT, preferred_element_type=jnp.float32)
            ue = lax.dot_general(a, e, FIRST, precision=EXACT, preferred_element_type=jnp.float32)
            left[o + BLOCK :, :] = left[o + BLOCK :, :] - ua[o + BLOCK :, :]
            right[o + BLOCK :, :] = right[o + BLOCK :, :] - ue[o + BLOCK :, :]
    return row <= col


def kernel(
    n_dp, n_rep, tokens, smap, test, basis, factor,
    tok, mp, tst, zt, yt, z, vb, send, pair, recv, p, left, right,
    in_sem, ps, pr, s1, r1, s2, r2, s3, r3,
):
    n = n_dp * n_rep
    m = n // 2
    dp = lax.axis_index("dp")
    rep = lax.axis_index("rep")
    b = lax.rem(rep, 2)
    g = lax.div(dp * n_rep + rep - b, 2)
    count, width = tok.shape
    k = mp.shape[1]
    slab = count // SLABS
    strip = width // n_dp

    test_copy = pltpu.make_async_copy(test.at[0, pl.ds(pl.multiple_of(dp * k, k), k)], tst, in_sem.at[2 * SLABS])
    loads = []
    for i in range(SLABS):
        part = pl.ds(i * slab, slab)
        loads.append(pltpu.make_async_copy(tokens.at[part], tok.at[part], in_sem.at[2 * i]))
        loads.append(pltpu.make_async_copy(smap.at[part], mp.at[part], in_sem.at[2 * i + 1]))
    for copy in loads:
        copy.start()
    test_copy.start()

    barrier = pltpu.get_barrier_semaphore()
    pl.semaphore_signal(barrier, inc=1, device_id=2 * g + 1 - b, device_id_type=LOGICAL)

    def greet(i, carry):
        peer = g + i
        peer = peer - jnp.where(peer >= m, m, 0)
        pl.semaphore_signal(barrier, inc=1, device_id=2 * peer + b, device_id_type=LOGICAL)
        return carry

    lax.fori_loop(1, m, greet, 0)

    for i in range(SLABS):
        loads[2 * i].wait()
        loads[2 * i + 1].wait()
        part = slice(i * slab, (i + 1) * slab)
        term = lax.dot_general(mp[part, :], tok[part, :], FIRST, preferred_element_type=jnp.float32)
        zt[...] = term if i == 0 else zt[...] + term
    test_copy.wait()
    span = width // 2

    def fill_start(side):
        part = zt[:, pl.ds(pl.multiple_of(side, k), span)].astype(jnp.bfloat16)
        z[pl.ds(side, span), :] = lax.dot_general(part, tst[...], FIRST, preferred_element_type=jnp.float32)

    def fill_power(side):
        part = tok[:, pl.ds(pl.multiple_of(side, k), span)]
        product = jnp.dot(yt[...], part, preferred_element_type=jnp.float32)
        for j in range(0, span, k):
            z[pl.ds(pl.multiple_of(side + j, 8), k), :] = product[:, j : j + k].T

    for stage in range(ITERS + 1):
        if stage > 0:
            for i in range(SLABS):
                part = slice(i * slab, (i + 1) * slab)
                y = jnp.dot(tok[part, :], vb[...], preferred_element_type=jnp.float32)
                yt[:, part] = y.T.astype(jnp.bfloat16)
        scale = 1.0 if stage == 0 else 1.0 / (count * n)
        finish = reduce_stage(
            n, b, g, scale, fill_power if stage else fill_start,
            (lambda: None) if stage else (lambda: pl.semaphore_wait(barrier, m)), z, send, pair.at[stage], recv.at[stage], p.at[stage],
            ps.at[stage], pr.at[stage], s1.at[stage], r1.at[stage], s2.at[stage], r2.at[stage],
            s3.at[stage], r3.at[stage],
        )
        upper = factorize(p.at[stage], left, right)
        if stage < ITERS:
            vb[...] = lax.dot_general(
                p[stage], right[...], LAST, precision=EXACT, preferred_element_type=jnp.float32
            ).astype(jnp.bfloat16)
        else:
            factor[...] = jnp.where(upper, left[...], 0.0)
            first = dp * strip
            if strip % 8 == 0:
                own = p[stage, pl.ds(pl.multiple_of(first, 8), strip), :]
            else:
                own = p[stage, pl.ds(first, strip), :]
            basis[...] = lax.dot_general(own, right[...], LAST, precision=EXACT, preferred_element_type=jnp.float32)
        finish()


def body(n_dp, n_rep, tokens, smap, test):
    n = n_dp * n_rep
    m = n // 2
    count, width = tokens.shape
    k = smap.shape[1]
    half = width // 2
    chunk = -(-half // (m * 8)) * 8
    owners = half // chunk
    stages = ITERS + 1
    dma = pltpu.SemaphoreType.DMA
    anywhere = pl.BlockSpec(memory_space=pl.ANY)
    vmem = pl.BlockSpec(memory_space=pltpu.VMEM)
    return pl.pallas_call(
        functools.partial(kernel, n_dp, n_rep),
        out_shape=(
            jax.ShapeDtypeStruct((width // n_dp, k), jnp.float32),
            jax.ShapeDtypeStruct((k, k), jnp.float32),
        ),
        in_specs=[anywhere] * 3,
        out_specs=(vmem, vmem),
        scratch_shapes=[
            pltpu.VMEM((count, width), jnp.bfloat16),
            pltpu.VMEM((count, k), jnp.bfloat16),
            pltpu.VMEM((k, k), jnp.bfloat16),
            pltpu.VMEM((k, width), jnp.float32),
            pltpu.VMEM((k, count), jnp.bfloat16),
            pltpu.VMEM((width, k), jnp.float32),
            pltpu.VMEM((width, k), jnp.bfloat16),
            pltpu.VMEM((owners, chunk, k), jnp.bfloat16),
            pltpu.VMEM((stages, half, k), jnp.float32),
            pltpu.VMEM((stages, m, chunk, k), jnp.bfloat16),
            pltpu.VMEM((stages, width, k), jnp.float32),
            pltpu.VMEM((k, k), jnp.float32),
            pltpu.VMEM((k, k), jnp.float32),
            dma((2 * SLABS + 1,)),
            dma((stages,)),
            dma((stages,)),
            dma((stages, m)),
            dma((stages, m)),
            dma((stages, m)),
            dma((stages, m)),
            dma((stages, m)),
            dma((stages, m)),
        ],
        compiler_params=pltpu.CompilerParams(collective_id=0, has_side_effects=True),
    )(tokens, smap, test)


def solution(mesh):
    return jax.shard_map(
        functools.partial(body, mesh.shape["dp"], mesh.shape["rep"]),
        mesh=mesh,
        in_specs=(P(("dp", "rep"), None), P(("dp", "rep"), None), P("rep", None, None)),
        out_specs=(P("dp", None), P()),
        check_vma=False,
    )
```
